256 devices in a mesh: agents: 64 (over z, x, core), group: 4 (over y).
Axes of the slice: x: 4, y: 4, z: 8, core: 2. Of those that a mesh axis runs over, the one named last changes fastest.
Arguments:
- q_lin: float32 [4, 40, 16384], P('group', None, 'agents'), may hold values from -6 to 6
- inverse: bfloat16 [4, 40, 40, 16384], P('group', None, None, 'agents'), may hold values from -0.5 to 1, as said below
- predict: bfloat16 [4, 40, 40, 16384], P('group', None, None, 'agents'), may hold values from -1 to 1
- free_traj: float32 [4, 40, 16384], P('group', None, 'agents'), may hold values from -6 to 6
- offsets: float32 [4, 8, 40, 16384], P('group', None, None, 'agents'), may hold values from -4 to 4
- multipliers: float32 [4, 8, 40, 16384], P('group', None, None, 'agents'), may hold values from -4 to 4
- nbr_owner: int32 [4, 8, 16384], P('group', None, 'agents'), may hold values from 0 to 63, as said below
- nbr_slot: int32 [4, 8, 16384], P('group', None, 'agents'), may hold values from -1 to 255
- platoon: int32 [4, 16384], P('group', 'agents'), may hold values from 0 to 127, as said below
Outputs:
- inputs_plan: float32 [4, 40, 16384], P('group', None, 'agents')
- multipliers_out: float32 [4, 8, 40, 16384], P('group', None, None, 'agents')
The draws below stay inside these ranges and needn't reach their ends.
Inputs may be any that keep to these rules, and one draw needn't show every extreme that they name: `nbr_owner`: an agent's own block index is its row in the region // 256; each neighbour's owner lies within 2 blocks of it, slot 0 is never padded. `inverse`: symmetric for every agent. `platoon`: 32 or more platoons hold no agent of any region.
All inputs are finite; a program needn't handle non-finite values. Where the reference program divides by a largest or mean magnitude, that divisor is 1e-20 or more.
Results may differ from the reference program's by a relative error of at most 0.0003.
Values sent between devices are 32-bit elements; how exact they have to be, the bound alone decides.
A program may use at most 64 MiB of HBM per device.

```python
import jax
import jax.numpy as jnp
from jax import lax

A_DEV = 256
QP = 40
TRAJ = 40
DEGREE = 8
SPAN = 2
NPLAT = 128
ITERS = 3
REGIONS = 4
PER = 16384


def neighbour_table(key):
    first, second, third = jax.random.split(jax.random.fold_in(key, 7), 3)
    shape = (REGIONS, DEGREE, PER)
    own = (jnp.arange(PER, dtype=jnp.int32) // A_DEV)[None, None, :]
    step = jax.random.randint(first, shape, -SPAN, SPAN + 1, dtype=jnp.int32)
    owner = jnp.clip(own + step, 0, PER // A_DEV - 1)
    slot = jax.random.randint(second, shape, 0, A_DEV, dtype=jnp.int32)
    alive = jax.random.randint(third, shape, 0, 4, dtype=jnp.int32) > 0
    alive = alive.at[:, 0, :].set(True)
    owner = jnp.where(alive, owner, own + jnp.zeros(shape, jnp.int32))
    slot = jnp.where(alive, slot, -1)
    return (owner, slot)


def draw_nbr_owner(key, part):
    return neighbour_table(key)[0]


def draw_nbr_slot(key, part):
    return neighbour_table(key)[1]


def draw_platoon(key, part):
    order_key, pick_key = jax.random.split(jax.random.fold_in(key, 13))
    order = jax.random.permutation(order_key, NPLAT).astype(jnp.int32)
    used = NPLAT - NPLAT // 4
    index = jax.random.randint(pick_key, (REGIONS, PER), 0, used, dtype=jnp.int32)
    return order[index].astype(jnp.int32)


def draw_inverse(key, part):
    noise_key = jax.random.fold_in(jax.random.fold_in(key, 11), 0)
    base = jax.random.normal(noise_key, (REGIONS, QP, QP, PER), jnp.float32) * 0.07
    sym = 0.5 * (base + jnp.transpose(base, (0, 2, 1, 3)))
    eye = jnp.eye(QP, dtype=jnp.float32)[None, :, :, None]
    whole = 0.5 * eye + sym
    return jnp.clip(whole, -0.5, 1.0).astype(jnp.bfloat16)


def levels(rng, extent, cuts, least, top_value):
    level, own = 1.0, jax.random.fold_in(rng, 6)
    for position, parts in cuts:
        heights = jnp.exp(jax.random.uniform(jax.random.fold_in(own, position), (parts,), jnp.float32, least / len(cuts), top_value / len(cuts)))
        level = level * jnp.repeat(heights, extent[position] // parts).reshape([-1 if axis == position else 1 for axis in range(len(extent))])
    return level


def scatter_about(own_key, extent, spread, most, shards=(), held_as=jnp.bfloat16):
    values = jax.random.normal(own_key, extent, jnp.float32) * spread
    if len(shards) > 0:
        values = levels(own_key, extent, shards, -0.22, 0.18) * values
    return jnp.clip(values, min=-most, max=most).astype(held_as)


def setup_inputs(seed: int = 0) -> dict:
    arg_keys = jax.random.split(jax.random.key(seed), 10)
    q_lin = scatter_about(arg_keys[0], (REGIONS, QP, PER), 1.0, 6.0, ((0, 4), (2, 64)), jnp.float32)
    inverse = draw_inverse(jax.random.fold_in(arg_keys[9], 71), 0)
    predict = scatter_about(arg_keys[2], (REGIONS, TRAJ, QP, PER), QP ** -0.5, 1.0, ((0, 4), (3, 64)))
    free_traj = scatter_about(arg_keys[3], (REGIONS, TRAJ, PER), 1.0, 6.0, ((0, 4), (2, 64)), jnp.float32)
    offsets = scatter_about(arg_keys[4], (REGIONS, DEGREE, TRAJ, PER), 0.5, 4.0, ((0, 4), (3, 64)), jnp.float32)
    multipliers = scatter_about(arg_keys[5], (REGIONS, DEGREE, TRAJ, PER), 0.5, 4.0, ((0, 4), (3, 64)), jnp.float32)
    nbr_owner = draw_nbr_owner(jax.random.fold_in(arg_keys[9], 71), 0)
    nbr_slot = draw_nbr_slot(jax.random.fold_in(arg_keys[9], 71), 0)
    platoon = draw_platoon(jax.random.fold_in(arg_keys[9], 71), 0)
    return {"q_lin": q_lin, "inverse": inverse, "predict": predict, "free_traj": free_traj, "offsets": offsets, "multipliers": multipliers, "nbr_owner": nbr_owner, "nbr_slot": nbr_slot, "platoon": platoon}


RHO = 0.5
KAPPA = 0.5


def lookup(field, nbr_owner, nbr_slot):
    live = nbr_slot >= 0
    column = jnp.where(live, nbr_owner * A_DEV + nbr_slot, 0).astype(jnp.int32)

    def one_region(rows, cols):
        taken = jnp.take(rows, cols.reshape(-1), axis=1)
        return taken.reshape(rows.shape[0], cols.shape[0], cols.shape[1])

    near = jax.vmap(one_region)(field, column)
    near = jnp.transpose(near, (0, 2, 1, 3))
    return near * live[:, :, None, :].astype(jnp.float32)


def platoon_pull(field, onehot):
    sums = jnp.einsum('rta,rpa->tp', field, onehot, precision=lax.Precision.HIGHEST)
    counts = jnp.sum(onehot, axis=(0, 2))
    means = sums / jnp.maximum(counts, 1.0)[None, :]
    return jnp.einsum('tp,rpa->rta', means, onehot, precision=lax.Precision.HIGHEST)


def reference(q_lin, inverse, predict, free_traj, offsets, multipliers, nbr_owner, nbr_slot, platoon):
    live = (nbr_slot >= 0).astype(jnp.float32)[:, :, None, :]
    onehot = (platoon[:, None, :] == jnp.arange(NPLAT, dtype=jnp.int32)[None, :, None]).astype(jnp.float32)
    inverse_wide = inverse.astype(jnp.float32)
    predict_wide = predict.astype(jnp.float32)
    traj = free_traj
    lam = multipliers
    near = lookup(traj, nbr_owner, nbr_slot)
    attract = platoon_pull(traj, onehot)
    plan = jnp.zeros_like(q_lin)
    for step in range(ITERS):
        coupling = jnp.sum(live * (lam - RHO * (near + offsets)), axis=1) - KAPPA * attract
        rhs = q_lin + jnp.einsum('rtja,rta->rja', predict_wide, coupling, precision=lax.Precision.HIGHEST)
        plan = -jnp.einsum('rija,rja->ria', inverse_wide, rhs, precision=lax.Precision.HIGHEST)
        traj = jnp.einsum('rtja,rja->rta', predict_wide, plan, precision=lax.Precision.HIGHEST) + free_traj
        near = lookup(traj, nbr_owner, nbr_slot)
        gap = live * (traj[:, None] - near - offsets)
        peak = jnp.max(jnp.abs(gap))
        lam = lam + gap / (1.0 + peak)
        if step + 1 < ITERS:
            attract = platoon_pull(traj, onehot)
    return plan, lam
```

```python
import functools

import jax
import jax.numpy as jnp
from jax import lax
from jax.experimental import pallas as pl
from jax.experimental.pallas import tpu as pltpu
from jax.sharding import Mesh
from jax.sharding import PartitionSpec as P

Z, X, Y = 8, 4, 4
BLOCKS = Z * X * 2
NB = 256
T = 40
DEGREE = 8
NPLAT = 128
ITERS = 3
RHO = 0.5
KAPPA = 0.5
TILES = T // 8
PEERS = 15
OFFS = (-2, -1, 1, 2)
AGENTS = ("agents_0", "agents_1", "agents_2")
MESH = pl.DeviceIdType.MESH
F32 = jnp.float32
HALVES = (slice(0, 128), slice(128, 256))


def kernel(
    q_h, inv_h, pre_h, free_h, off_h, lam_h, own_h, slot_h, plat_h,
    plan_o, lam_o,
    q_v, inv_b, pre_b, off_v, lam_v, gap_v, near_v, own_v, slot_v, plat_v,
    col_v, low_v, hot_v, inv_f, pre_f, traj_v, nbr_v, c0_v, c1_v, vec_v, plan_v, att_v, div_v,
    s_buf, a_buf, m_buf, b_buf, e_buf, c_buf, p_src, p1_buf, p2_buf,
    in_sem, out_sem, nbr_ss, nbr_rs, a_ss, a_rs, b_ss, b_rs, c_ss, c_rs, p_ss, p_rs,
):
    z = lax.axis_index("agents_0")
    x = lax.axis_index("agents_1")
    core = lax.axis_index("agents_2")
    y = lax.axis_index("group")
    mine = (z * X + x) * 2 + core
    u = z * 2 + core
    v = x * Y + y

    loads = [
        pltpu.make_async_copy(src, dst, in_sem.at[i])
        for i, (src, dst) in enumerate(
            (
                (free_h, traj_v.at[0]),
                (plat_h, plat_v),
                (own_h, own_v),
                (slot_h, slot_v),
                (off_h, off_v),
                (lam_h, lam_v),
                (pre_h, pre_b),
                (q_h, q_v),
                (inv_h, inv_b),
            )
        )
    ]
    for load in loads:
        load.start()

    def at_block(b):
        return {"agents_0": b // (2 * X), "agents_1": (b // 2) % X, "agents_2": b % 2}

    def at_u(w):
        return {"agents_0": w // 2, "agents_2": w % 2}

    def at_v(w):
        return {"agents_1": w // Y, "group": w % Y}

    near_ids = [at_block(lax.rem(mine - d + BLOCKS, BLOCKS)) for d in OFFS]
    u_ids = [at_u(lax.rem(u + d, 16)) for d in range(1, 16)]
    v_ids = [at_v(lax.rem(v + d, 16)) for d in range(1, 16)]

    barrier = pltpu.get_barrier_semaphore()
    for ids in near_ids + u_ids + v_ids:
        pl.semaphore_signal(barrier, inc=1, device_id=ids, device_id_type=MESH)

    def remote(src, dst, ss, rs, ids):
        return pltpu.make_async_remote_copy(
            src_ref=src, dst_ref=dst, send_sem=ss, recv_sem=rs, device_id=ids, device_id_type=MESH
        )

    def whole_wait(ref, sem):
        pltpu.make_async_copy(ref, ref, sem).wait()

    def nbr_send(i):
        for j, ids in enumerate(near_ids):
            remote(traj_v.at[i], nbr_v.at[i, j], nbr_ss.at[i, j], nbr_rs.at[i, j], ids).start()

    def platoon_tiles(i):
        field = traj_v[i]
        hi = field.astype(jnp.bfloat16)
        rest = field - hi.astype(F32)
        mid = rest.astype(jnp.bfloat16)
        low = (rest - mid.astype(F32)).astype(jnp.bfloat16)
        total = jnp.zeros((T, NPLAT), F32)
        for part in (low, mid, hi):
            total += lax.dot_general(
                part, hot_v[...], (((1,), (1,)), ((), ())), preferred_element_type=F32
            )
        for g in range(TILES):
            s_buf[i, g] = total[8 * g : 8 * g + 8]

    def owner_of(tiles):
        return jnp.logical_and(core == 1, z < tiles)

    def sum_send(i, tiles):
        for g in range(tiles):
            owner = 2 * g + 1

            @pl.when(u != owner)
            def _():
                slot = lax.rem(u - owner + 16, 16) - 1
                remote(
                    s_buf.at[i, g], a_buf.at[i, slot], a_ss.at[i, g], a_rs.at[i],
                    {"agents_0": g, "agents_2": 1},
                ).start()

    def sum_mid(i, tiles):
        @pl.when(owner_of(tiles))
        def _():
            whole_wait(a_buf.at[i], a_rs.at[i])
            m_buf[i] = s_buf[i, z] + jnp.sum(a_buf[i], axis=0)
            for d in range(PEERS):
                remote(m_buf.at[i], b_buf.at[i, d], b_ss.at[i], b_rs.at[i], v_ids[d]).start()

    def sum_end(i, tiles):
        @pl.when(owner_of(tiles))
        def _():
            whole_wait(b_buf.at[i], b_rs.at[i])
            total = m_buf[i] + jnp.sum(b_buf[i], axis=0)
            e_buf[i] = total
            c_buf[i, z] = total
            for d in range(PEERS):
                remote(e_buf.at[i], c_buf.at[i, z], c_ss.at[i], c_rs.at[i, z], u_ids[d]).start()

        for g in range(tiles):

            @pl.when(u != 2 * g + 1)
            def _():
                whole_wait(c_buf.at[i, g], c_rs.at[i, g])

    def sum_drain(i, tiles):
        for g in range(tiles):

            @pl.when(u != 2 * g + 1)
            def _():
                whole_wait(s_buf.at[i, g], a_ss.at[i, g])

        @pl.when(owner_of(tiles))
        def _():
            whole_wait(b_buf.at[i], b_ss.at[i])
            whole_wait(a_buf.at[i], c_ss.at[i])

    def peak_first(i, peak):
        p_src[i, 0] = peak
        for d in range(PEERS):
            remote(p_src.at[i, 0], p1_buf.at[i, d], p_ss.at[i, 0], p_rs.at[i, 0], u_ids[d]).start()

    def peak_second(i):
        whole_wait(p1_buf.at[i], p_rs.at[i, 0])
        p_src[i, 1] = jnp.maximum(p_src[i, 0], jnp.max(p1_buf[i], axis=0))
        for d in range(PEERS):
            remote(p_src.at[i, 1], p2_buf.at[i, d], p_ss.at[i, 1], p_rs.at[i, 1], v_ids[d]).start()

    def peak_end(i):
        whole_wait(p2_buf.at[i], p_rs.at[i, 1])
        peak = jnp.maximum(p_src[i, 1], jnp.max(p2_buf[i], axis=0))
        return 1.0 / (1.0 + jnp.max(peak, axis=1, keepdims=True))

    def peak_drain(i):
        whole_wait(p1_buf.at[i], p_ss.at[i, 0])
        whole_wait(p2_buf.at[i], p_ss.at[i, 1])

    def row(ref, k, half):
        return jnp.concatenate([ref[k, :, half]] * TILES, axis=0)

    def pick(src, block, col, low, other):
        first = jnp.take_along_axis(src[0], low, axis=1, mode="promise_in_bounds")
        second = jnp.take_along_axis(src[1], low, axis=1, mode="promise_in_bounds")
        return jnp.where(col == 2 * block, first, jnp.where(col == 2 * block + 1, second, other))

    def look(ref, block, fresh):
        src = [ref[:, half] for half in HALVES]

        def body(k, carry):
            for half in HALVES:
                other = 0.0 if fresh else near_v[k, :, half]
                near_v[k, :, half] = pick(src, block, row(col_v, k, half), row(low_v, k, half), other)
            return carry

        lax.fori_loop(0, DEGREE, body, 0)

    def gather_all(i, s_prev):
        look(traj_v.at[i], 2, True)
        for j, block in ((1, 1), (2, 3), (0, 0)):
            whole_wait(nbr_v.at[i, j], nbr_rs.at[i, j])
            look(nbr_v.at[i, j], block, False)
        whole_wait(nbr_v.at[i, 3], nbr_rs.at[i, 3])
        src = [nbr_v[i, 3, :, half] for half in HALVES]
        top = jnp.zeros((T, 128), F32)
        zero = jnp.zeros((T, 128), F32)
        for half in HALVES:
            here = traj_v[i, :, half]

            def body(k, carry):
                c0, c1, top = carry
                col = row(col_v, k, half)
                near = pick(src, 4, col, row(low_v, k, half), near_v[k, :, half])
                off = off_v[k, :, half]
                lam = lam_v[k, :, half]
                if i > 1:
                    lam = lam + s_prev * gap_v[k, :, half]
                    lam_v[k, :, half] = lam
                live = col >= 0
                c0 = c0 + jnp.where(live, lam - RHO * (near + off), 0.0)
                if i > 0:
                    gap = jnp.where(live, here - near - off, 0.0)
                    gap_v[k, :, half] = gap
                    c1 = c1 + gap
                    top = jnp.maximum(top, jnp.abs(gap))
                return c0, c1, top

            c0, c1, top = lax.fori_loop(0, DEGREE, body, (zero, zero, top))
            c0_v[:, half] = c0
            c1_v[:, half] = c1
        return jnp.max(top, axis=0, keepdims=True)

    def contract(mat, vec):
        def body(g, acc):
            at = pl.multiple_of(g * 8, 8)
            part = vec[pl.ds(at, 8), :]
            for r in range(8):
                acc = acc + mat[at + r] * part[r : r + 1]
            return acc

        return lax.fori_loop(0, TILES, body, jnp.zeros((T, NB), F32))

    def predict(i):
        plan = plan_v[...]

        def body(g, carry):
            at = pl.multiple_of(g * 8, 8)
            rows = [jnp.sum(pre_f[at + r] * plan, axis=0, keepdims=True) for r in range(8)]
            traj_v[i, pl.ds(at, 8), :] = jnp.concatenate(rows, axis=0) + traj_v[0, pl.ds(at, 8), :]
            return carry

        lax.fori_loop(0, TILES, body, 0)

    def attract(i):
        for half in HALVES:
            index = jnp.broadcast_to(plat_v[:, half], (T, 128))
            means = c_buf[i, 0:TILES].reshape(T, NPLAT) / div_v[...]
            att_v[:, half] = jnp.take_along_axis(means, index, axis=1, mode="promise_in_bounds")

    loads[0].wait()
    pl.semaphore_wait(barrier, len(near_ids) + 2 * PEERS)
    nbr_send(0)
    loads[1].wait()
    match = lax.broadcasted_iota(jnp.int32, (NPLAT, NB), 0) == plat_v[...]
    hot_v[...] = match.astype(F32).astype(jnp.bfloat16)
    ones = jnp.ones((8, NB), jnp.bfloat16)
    s_buf[0, TILES] = lax.dot_general(
        ones, hot_v[...], (((1,), (1,)), ((), ())), preferred_element_type=F32
    )
    platoon_tiles(0)
    sum_send(0, TILES + 1)
    loads[2].wait()
    loads[3].wait()
    slot = slot_v[...]
    low = slot & 127
    col = jnp.where(slot >= 0, (own_v[...] - mine + 2) * 2 + (slot >> 7), -1)
    for k in range(DEGREE):
        low_v[k] = jnp.broadcast_to(low[k : k + 1], (8, NB))
        col_v[k] = jnp.broadcast_to(col[k : k + 1], (8, NB))
    loads[4].wait()
    loads[5].wait()
    gather_all(0, None)
    sum_mid(0, TILES + 1)
    for load in loads[6:]:
        load.wait()

    def widen(t, carry):
        inv_f[t] = inv_b[t].astype(F32)
        pre_f[t] = pre_b[t].astype(F32)
        return carry

    lax.fori_loop(0, T, widen, 0)
    sum_end(0, TILES + 1)
    div_v[...] = jnp.broadcast_to(jnp.maximum(c_buf[0, TILES, 0:1], 1.0), (T, NPLAT))
    attract(0)

    s = None
    for step in range(ITERS):
        i = step + 1
        more = i < ITERS
        coupling = c0_v[...] - KAPPA * att_v[...]
        if step > 0:
            coupling = coupling + s * c1_v[...]
        vec_v[...] = coupling
        vec_v[...] = q_v[...] + contract(pre_f, vec_v)
        plan_v[...] = -contract(inv_f, vec_v)
        predict(i)
        nbr_send(i)
        if more:
            platoon_tiles(i)
            sum_send(i, TILES)
        else:
            pltpu.make_async_copy(plan_v, plan_o, out_sem.at[DEGREE]).start()
        peak = gather_all(i, s)
        peak_first(step, peak)
        if more:
            sum_mid(i, TILES)
        peak_second(step)
        if more:
            sum_end(i, TILES)
            attract(i)
        s = peak_end(step)

    for k in range(DEGREE):
        lam_v[k] = lam_v[k] + s * gap_v[k]
        pltpu.make_async_copy(lam_v.at[k], lam_o.at[k], out_sem.at[k]).start()
    for i in range(ITERS + 1):
        for j in range(len(OFFS)):
            whole_wait(traj_v.at[i], nbr_ss.at[i, j])
    for i in range(ITERS):
        sum_drain(i, TILES + 1 if i == 0 else TILES)
        peak_drain(i)
    for k in range(DEGREE):
        pltpu.make_async_copy(lam_v.at[k], lam_o.at[k], out_sem.at[k]).wait()
    pltpu.make_async_copy(plan_v, plan_o, out_sem.at[DEGREE]).wait()


def local(q_lin, inverse, predict, free_traj, offsets, multipliers, nbr_owner, nbr_slot, platoon):
    vm = pltpu.VMEM
    i32, bf16 = jnp.int32, jnp.bfloat16
    dma = pltpu.SemaphoreType.DMA
    field = (T, NB)
    slots = (DEGREE, T, NB)
    mats = (T, T, NB)
    plan, lam = pl.pallas_call(
        kernel,
        out_shape=(jax.ShapeDtypeStruct(field, F32), jax.ShapeDtypeStruct(slots, F32)),
        in_specs=[pl.BlockSpec(memory_space=pl.ANY)] * 9,
        out_specs=(pl.BlockSpec(memory_space=pl.ANY), pl.BlockSpec(memory_space=pl.ANY)),
        scratch_shapes=[
            vm(field, F32), vm(mats, bf16), vm(mats, bf16), vm(slots, F32), vm(slots, F32),
            vm(slots, F32), vm(slots, F32), vm((DEGREE, NB), i32), vm((DEGREE, NB), i32), vm((1, NB), i32),
            vm((DEGREE, 8, NB), i32), vm((DEGREE, 8, NB), i32), vm((NPLAT, NB), bf16), vm(mats, F32), vm(mats, F32),
            vm((ITERS + 1, T, NB), F32), vm((ITERS + 1, 4, T, NB), F32),
            vm(field, F32), vm(field, F32), vm(field, F32), vm(field, F32), vm(field, F32), vm((T, NPLAT), F32),
            vm((ITERS, TILES + 1, 8, 128), F32), vm((ITERS, PEERS, 8, 128), F32), vm((ITERS, 8, 128), F32),
            vm((ITERS, PEERS, 8, 128), F32), vm((ITERS, 8, 128), F32), vm((ITERS, TILES + 1, 8, 128), F32),
            vm((ITERS, 2, 1, 128), F32), vm((ITERS, PEERS, 1, 128), F32), vm((ITERS, PEERS, 1, 128), F32),
            dma((9,)), dma((DEGREE + 1,)), dma((ITERS + 1, 4)), dma((ITERS + 1, 4)),
            dma((ITERS, TILES + 1)), dma((ITERS,)), dma((ITERS,)), dma((ITERS,)), dma((ITERS,)),
            dma((ITERS, TILES + 1)), dma((ITERS, 2)), dma((ITERS, 2)),
        ],
        compiler_params=pltpu.CompilerParams(collective_id=0, has_side_effects=True),
        name="consensus",
    )(
        q_lin[0], inverse[0], predict[0], free_traj[0], offsets[0], multipliers[0],
        nbr_owner[0], nbr_slot[0], platoon,
    )
    return plan[None], lam[None]


def solution(mesh):
    finer = Mesh(
        mesh.devices.reshape(Z, X, 2, mesh.shape["group"]),
        ("agents_0", "agents_1", "agents_2", "group"),
    )
    placed = (
        P("group", None, AGENTS),
        P("group", None, None, AGENTS),
        P("group", None, None, AGENTS),
        P("group", None, AGENTS),
        P("group", None, None, AGENTS),
        P("group", None, None, AGENTS),
        P("group", None, AGENTS),
        P("group", None, AGENTS),
        P("group", AGENTS),
    )
    return jax.shard_map(
        local,
        mesh=finer,
        in_specs=placed,
        out_specs=(P("group", None, AGENTS), P("group", None, None, AGENTS)),
        check_vma=False,
    )
```
